16 devices in a mesh: dp: 4 (over z, y), tp: 4 (over x, core).
Axes of the slice: x: 2, y: 2, z: 2, core: 2. Of those that a mesh axis runs over, the one named last changes fastest.
Arguments:
- hidden: bfloat16 [8, 1024, 5120], P('dp', 'tp'), parts along dimension 0
- positions: int32 [8, 1024], P('dp'), parts along dimension 0
- gain_attn: bfloat16 [5120], replicated
- w_q: bfloat16 [5120, 5120], P(None, 'tp')
- b_q: bfloat16 [5120], P('tp')
- w_k: bfloat16 [5120, 1024], P(None, 'tp')
- b_k: bfloat16 [1024], P('tp')
- w_v: bfloat16 [5120, 1024], P(None, 'tp')
- b_v: bfloat16 [1024], P('tp')
- w_o: bfloat16 [5120, 5120], P('tp')
- gain_mlp: bfloat16 [5120], replicated
- w_gate: bfloat16 [5120, 27648], P(None, 'tp')
- w_up: bfloat16 [5120, 27648], P(None, 'tp')
- w_down: bfloat16 [27648, 5120], P('tp')
Outputs:
- output 1: bfloat16 [8, 1024, 5120], P('dp', 'tp'), parts along dimension 0
- output 2: bfloat16 [8, 1024, 8, 128], P('dp', None, 'tp'), parts along dimension 0
- output 3: bfloat16 [8, 1024, 8, 128], P('dp', None, 'tp'), parts along dimension 0
There are 4 independent parts. The reference program is written for one: setup_inputs(seed, part) draws one part's arguments, and reference() takes and returns one part's arrays. A program takes and returns all parts, laid end to end along the dimension named above; an argument that names none is the same for every part.
All inputs are finite; a program needn't handle non-finite values.
Results may differ from the reference program's by a relative error of at most 0.0130781.
Values are sent between devices in bfloat16 or wider.
A program may use at most 1 GiB of HBM per device.

```python
import jax
import jax.numpy as jnp
from jax import lax

N_BATCH = 2
SEQ_LEN = 1024
D_MODEL = 5120
N_HEADS = 40
N_KV_HEADS = 8
HEAD_DIM = 128
FF_DIM = 27648

GROUP_SIZE = N_HEADS // N_KV_HEADS
ROPE_THETA = 1000000.0
NORM_EPS = 1e-6


def normal_draw(rng_key, shape, scale):
    return (jax.random.normal(rng_key, shape, jnp.float32) * scale).astype(jnp.bfloat16)


def gain_draw(rng_key):
    return (0.5 + jax.random.uniform(rng_key, (D_MODEL,), jnp.float32)).astype(jnp.bfloat16)


def setup_inputs(seed: int = 0, part: int = 0) -> dict:
    base_key = jax.random.key(seed)
    part_key = jax.random.fold_in(base_key, part)
    hidden_key, start_key = jax.random.split(part_key, 2)
    key_list = jax.random.split(base_key, 12)
    q_width = N_HEADS * HEAD_DIM
    kv_width = N_KV_HEADS * HEAD_DIM
    start_pos = jax.random.randint(start_key, (N_BATCH, 1), 0, 2 * SEQ_LEN, dtype=jnp.int32)
    return {
        'hidden': normal_draw(hidden_key, (N_BATCH, SEQ_LEN, D_MODEL), 1.0),
        'positions': start_pos + jnp.arange(SEQ_LEN, dtype=jnp.int32)[None, :],
        'gain_attn': gain_draw(key_list[0]),
        'w_q': normal_draw(key_list[1], (D_MODEL, q_width), 1.5 * D_MODEL ** -0.5),
        'b_q': normal_draw(key_list[2], (q_width,), 0.3),
        'w_k': normal_draw(key_list[3], (D_MODEL, kv_width), 1.5 * D_MODEL ** -0.5),
        'b_k': normal_draw(key_list[4], (kv_width,), 0.3),
        'w_v': normal_draw(key_list[5], (D_MODEL, kv_width), D_MODEL ** -0.5),
        'b_v': normal_draw(key_list[6], (kv_width,), 0.3),
        'w_o': normal_draw(key_list[7], (q_width, D_MODEL), q_width ** -0.5),
        'gain_mlp': gain_draw(key_list[8]),
        'w_gate': normal_draw(key_list[9], (D_MODEL, FF_DIM), D_MODEL ** -0.5),
        'w_up': normal_draw(key_list[10], (D_MODEL, FF_DIM), D_MODEL ** -0.5),
        'w_down': normal_draw(key_list[11], (FF_DIM, D_MODEL), FF_DIM ** -0.5),
    }


def rms_norm(values, gain):
    values_f32 = values.astype(jnp.float32)
    inv_rms = lax.rsqrt(jnp.mean(values_f32 * values_f32, axis=-1, keepdims=True) + NORM_EPS)
    return (values_f32 * inv_rms * gain.astype(jnp.float32)).astype(jnp.bfloat16)


def rotary(values, positions):
    half_dim = HEAD_DIM // 2
    inv_freq = ROPE_THETA ** (-jnp.arange(half_dim, dtype=jnp.float32) / half_dim)
    angles = positions.astype(jnp.float32)[:, :, None] * inv_freq
    angles = angles.reshape(angles.shape[:2] + (1,) * (values.ndim - 3) + (half_dim,))
    cosine = jnp.cos(angles)
    sine = jnp.sin(angles)
    first = values[..., :half_dim]
    second = values[..., half_dim:]
    return jnp.concatenate([first * cosine - second * sine, second * cosine + first * sine], axis=-1)


def reference(hidden, positions, gain_attn, w_q, b_q, w_k, b_k, w_v, b_v, w_o, gain_mlp, w_gate, w_up, w_down):
    tokens = N_BATCH * SEQ_LEN
    normed = rms_norm(hidden, gain_attn).reshape(tokens, D_MODEL)
    query = jnp.dot(normed, w_q, preferred_element_type=jnp.float32) + b_q.astype(jnp.float32)
    key_proj = jnp.dot(normed, w_k, preferred_element_type=jnp.float32) + b_k.astype(jnp.float32)
    value_proj = jnp.dot(normed, w_v, preferred_element_type=jnp.float32) + b_v.astype(jnp.float32)
    query = rotary(query.reshape(N_BATCH, SEQ_LEN, N_HEADS, HEAD_DIM), positions).astype(jnp.bfloat16)
    k_cache = rotary(key_proj.reshape(N_BATCH, SEQ_LEN, N_KV_HEADS, HEAD_DIM), positions).astype(jnp.bfloat16)
    v_cache = value_proj.reshape(N_BATCH, SEQ_LEN, N_KV_HEADS, HEAD_DIM).astype(jnp.bfloat16)
    query_groups = query.reshape(N_BATCH, SEQ_LEN, N_KV_HEADS, GROUP_SIZE, HEAD_DIM).transpose(0, 2, 1, 3, 4).reshape(N_BATCH * N_KV_HEADS, SEQ_LEN, GROUP_SIZE, HEAD_DIM)
    key_groups = k_cache.transpose(0, 2, 1, 3).reshape(N_BATCH * N_KV_HEADS, SEQ_LEN, HEAD_DIM)
    value_groups = v_cache.transpose(0, 2, 1, 3).reshape(N_BATCH * N_KV_HEADS, SEQ_LEN, HEAD_DIM)
    causal = jnp.arange(SEQ_LEN)[:, None] >= jnp.arange(SEQ_LEN)[None, :]
    score_scale = HEAD_DIM ** -0.5

    def attend(operands):
        q_grp, k_grp, v_grp = operands
        scores = jnp.einsum('tgd,sd->gts', q_grp.astype(jnp.float32), k_grp.astype(jnp.float32)) * score_scale
        scores = jnp.where(causal[None], scores, -1e30)
        attn_probs = jax.nn.softmax(scores, axis=-1).astype(jnp.bfloat16).astype(jnp.float32)
        return jnp.einsum('gts,sd->tgd', attn_probs, v_grp.astype(jnp.float32)).astype(jnp.bfloat16)

    attn_out = lax.map(attend, (query_groups, key_groups, value_groups))
    attn_out = attn_out.reshape(N_BATCH, N_KV_HEADS, SEQ_LEN, GROUP_SIZE, HEAD_DIM).transpose(0, 2, 1, 3, 4).reshape(tokens, N_HEADS * HEAD_DIM)
    residual = hidden.reshape(tokens, D_MODEL).astype(jnp.float32)
    hidden_mid = (residual + jnp.dot(attn_out, w_o, preferred_element_type=jnp.float32)).astype(jnp.bfloat16)
    normed_mid = rms_norm(hidden_mid, gain_mlp)
    gate = jnp.dot(normed_mid, w_gate, preferred_element_type=jnp.float32)
    up_proj = jnp.dot(normed_mid, w_up, preferred_element_type=jnp.float32)
    activation = (jax.nn.silu(gate) * up_proj).astype(jnp.bfloat16)
    down_proj = jnp.dot(activation, w_down, preferred_element_type=jnp.float32)
    hidden_out = (hidden_mid.astype(jnp.float32) + down_proj).astype(jnp.bfloat16)
    return (hidden_out.reshape(N_BATCH, SEQ_LEN, D_MODEL), k_cache, v_cache)
```

```python
import functools

import jax
import jax.numpy as jnp
from jax import lax
from jax.experimental import pallas as pl
from jax.experimental.pallas import tpu as pltpu
from jax.sharding import PartitionSpec as P

HEAD_DIM = 128
ROPE_THETA = 1000000.0
NORM_EPS = 1e-6
Q_BLOCK = 256
DOWN_SPLIT = 4


def rms_norm(values, gain):
    values_f32 = values.astype(jnp.float32)
    inv_rms = lax.rsqrt(jnp.mean(values_f32 * values_f32, axis=-1, keepdims=True) + NORM_EPS)
    return (values_f32 * inv_rms * gain.astype(jnp.float32)).astype(jnp.bfloat16)


def rope_tables(positions):
    half_dim = HEAD_DIM // 2
    inv_freq = ROPE_THETA ** (-jnp.arange(half_dim, dtype=jnp.float32) / half_dim)
    angles = positions.astype(jnp.float32)[:, None] * inv_freq
    cosine = jnp.cos(angles)
    sine = jnp.sin(angles)
    return jnp.concatenate([cosine, cosine], axis=-1), jnp.concatenate([-sine, sine], axis=-1)


def attention_kernel(cos_ref, sin_ref, q_ref, k_ref, v_ref, o_ref, k_out_ref, q_rot):
    seq_len = q_ref.shape[0]

    def rotate(values):
        return values * cos_ref[...] + pltpu.roll(values, HEAD_DIM // 2, 1) * sin_ref[...]

    @pl.when(pl.program_id(1) == 0)
    def _():
        k_out_ref[...] = rotate(k_ref[...]).astype(jnp.bfloat16)

    q_rot[...] = rotate(q_ref[...]).astype(jnp.bfloat16)
    scale = HEAD_DIM ** -0.5
    dims = (((1,), (1,)), ((), ()))
    rows = lax.broadcasted_iota(jnp.int32, (Q_BLOCK, Q_BLOCK), 0)
    cols = lax.broadcasted_iota(jnp.int32, (Q_BLOCK, Q_BLOCK), 1)
    causal = rows >= cols
    for i in range(seq_len // Q_BLOCK):
        lo, hi = i * Q_BLOCK, (i + 1) * Q_BLOCK
        q = q_rot[lo:hi, :]
        diag = lax.dot_general(q, k_out_ref[lo:hi, :], dims, preferred_element_type=jnp.float32) * scale
        diag = jnp.where(causal, diag, -1e30)
        top = jnp.max(diag, axis=-1, keepdims=True)
        if i:
            past = lax.dot_general(q, k_out_ref[:lo, :], dims, preferred_element_type=jnp.float32) * scale
            top = jnp.maximum(top, jnp.max(past, axis=-1, keepdims=True))
        diag = jnp.exp(diag - top)
        norm = jnp.sum(diag, axis=-1, keepdims=True)
        if i:
            past = jnp.exp(past - top)
            norm = norm + jnp.sum(past, axis=-1, keepdims=True)
        inv = 1.0 / norm
        out = jnp.dot((diag * inv).astype(jnp.bfloat16), v_ref[lo:hi, :], preferred_element_type=jnp.float32)
        if i:
            out = out + jnp.dot((past * inv).astype(jnp.bfloat16), v_ref[:lo, :], preferred_element_type=jnp.float32)
        o_ref[lo:hi, :] = out.astype(jnp.bfloat16)


def attention(cosine, sine, query, key, value):
    seq_len, q_width = query.shape
    kv_width = key.shape[1]
    group = q_width // kv_width
    kv_heads = kv_width // HEAD_DIM
    full = pl.BlockSpec((seq_len, HEAD_DIM), lambda h, g: (0, 0))
    per_q = pl.BlockSpec((seq_len, HEAD_DIM), lambda h, g: (0, h * group + g))
    per_kv = pl.BlockSpec((seq_len, HEAD_DIM), lambda h, g: (0, h))
    return pl.pallas_call(
        attention_kernel,
        grid=(kv_heads, group),
        in_specs=[full, full, per_q, per_kv, per_kv],
        out_specs=[per_q, per_kv],
        out_shape=[jax.ShapeDtypeStruct((seq_len, q_width), jnp.bfloat16),
                   jax.ShapeDtypeStruct((seq_len, kv_width), jnp.bfloat16)],
        scratch_shapes=[pltpu.VMEM((seq_len, HEAD_DIM), jnp.bfloat16)],
        compiler_params=pltpu.CompilerParams(vmem_limit_bytes=32 * 1024 * 1024),
        cost_estimate=pl.CostEstimate(flops=16 * seq_len * seq_len * q_width, bytes_accessed=8 * seq_len * q_width, transcendentals=0),
        name="attention",
    )(cosine, sine, query, key, value)


def after(value, *others):
    return lax.optimization_barrier((value,) + others)[0]


def dot(left, right):
    return jnp.dot(left, right, preferred_element_type=jnp.float32)


def solution(mesh):
    def local_layer(hidden, positions, gain_attn, w_q, b_q, w_k, b_k, w_v, b_v, w_o, gain_mlp, w_gate, w_up, w_down):
        batch = hidden.shape[0]
        seq_len = positions.shape[1]
        kv_local = w_k.shape[1] // HEAD_DIM
        width = hidden.shape[2]

        def gather(part):
            return lax.all_gather(part, 'tp', axis=0, tiled=True)

        def scatter(part):
            return lax.psum_scatter(part, 'tp', scatter_dimension=0, tiled=True)

        def bias(vec):
            return vec.astype(jnp.float32)

        def add(res, total):
            return (res.astype(jnp.float32) + total.astype(jnp.float32)).astype(jnp.bfloat16)

        def qkv_attention(x, tables):
            query = dot(x, w_q) + bias(b_q)
            key = dot(x, w_k) + bias(b_k)
            value = (dot(x, w_v) + bias(b_v)).astype(jnp.bfloat16)
            out, key = attention(tables[0], tables[1], query, key, value)
            return out, key, value

        tables = [rope_tables(positions[b]) for b in range(batch)]
        normed0 = rms_norm(hidden[0], gain_attn)
        x0 = gather(normed0)
        normed1 = rms_norm(after(hidden[1], normed0), gain_attn)
        x1 = gather(normed1)
        o0, k0, v0 = qkv_attention(x0, tables[0])
        rows = hidden.shape[1]
        half = rows // 2

        def half_of(values, i):
            parts = values.reshape(seq_len // rows, rows, -1)
            return parts[:, i * half:(i + 1) * half].reshape(seq_len // 2, -1)

        part00 = dot(half_of(o0, 0), w_o).astype(jnp.bfloat16)
        sum00 = scatter(part00)
        part01 = dot(after(half_of(o0, 1), part00), w_o).astype(jnp.bfloat16)
        sum01 = scatter(part01)
        o1, k1, v1 = qkv_attention(after(x1, part01), tables[1])
        mid00 = add(hidden[0, :half], after(sum00, o1))
        h00 = rms_norm(mid00, gain_mlp)
        y00 = gather(h00)
        mid01 = add(hidden[0, half:], after(sum01, h00))
        h01 = rms_norm(mid01, gain_mlp)
        y01 = gather(h01)
        part1 = dot(after(o1, h01), w_o).astype(jnp.bfloat16)
        sum1 = scatter(part1)
        y00 = after(y00, part1)
        gate00 = dot(y00, w_gate)
        up00 = dot(after(y00, gate00), w_up)
        act00 = (jax.nn.silu(gate00) * up00).astype(jnp.bfloat16)
        y01 = after(y01, act00)
        gate01 = dot(y01, w_gate)
        mid1 = add(hidden[1], after(sum1, gate01))
        h1 = rms_norm(mid1, gain_mlp)
        y1 = gather(h1)
        up01 = dot(after(y01, h1), w_up)
        act01 = (jax.nn.silu(gate01) * up01).astype(jnp.bfloat16)
        down00 = dot(after(act00, act01), w_down).astype(jnp.bfloat16)
        total00 = scatter(after(down00, y1))
        down0 = dot(after(act01, down00), w_down).astype(jnp.bfloat16)
        total0 = scatter(after(down0, total00))
        y1 = after(y1, down0)
        gate1 = dot(y1, w_gate)
        up1 = dot(y1, w_up)
        act1 = (jax.nn.silu(gate1) * up1).astype(jnp.bfloat16)
        out0 = jnp.concatenate([add(mid00, after(total00, act1)), add(mid01, after(total0, act1))], axis=0)
        step = width // DOWN_SPLIT
        outs = []
        previous = total0
        for i in range(DOWN_SPLIT):
            cols = slice(i * step, (i + 1) * step)
            down = dot(act1, w_down[:, cols]).astype(jnp.bfloat16)
            act1 = after(act1, down)
            previous = scatter(after(down, previous))
            outs.append(add(mid1[:, cols], previous))
        out1 = jnp.concatenate(outs, axis=1)
        shape = (seq_len, kv_local, HEAD_DIM)
        stack = lambda a, b: jnp.stack([a.reshape(shape), b.reshape(shape)])
        return jnp.stack([out0, out1]), stack(k0, k1), stack(v0, v1)

    token_rows = P('dp', 'tp', None)
    col_split = P(None, 'tp')
    row_split = P('tp', None)
    vec_split = P('tp')
    replicated = P(None)
    cache_spec = P('dp', None, 'tp', None)
    in_specs = (token_rows, P('dp', None), replicated, col_split, vec_split, col_split, vec_split, col_split, vec_split, row_split, replicated, col_split, col_split, row_split)
    out_specs = (token_rows, cache_spec, cache_spec)
    return jax.shard_map(local_layer, mesh=mesh, in_specs=in_specs, out_specs=out_specs, check_vma=False)
```
